32 devices in a mesh: rows: 32 (over z, y, x, core).
Axes of the slice: x: 2, y: 2, z: 4, core: 2. Of those that a mesh axis runs over, the one named last changes fastest.
Arguments:
- events: float32 [4, 32, 262144], P(None, None, 'rows'), may hold values from -8 to 8
- keep_indicator: int32 [4, 262144], P(None, 'rows'), may hold values from 0 to 1, as said below
Outputs:
- lagging_mean: float32 [4, 32, 262144], P(None, None, 'rows')
- deviation: float32 [4, 32, 262144], P(None, None, 'rows')
The draws below stay inside these ranges and needn't reach their ends.
Inputs may be any that keep to these rules, and one draw needn't show every extreme that they name: `keep_indicator`: in each table, each of the 32 aligned blocks of 8192 rows holds at least 4096 survivors, and some block holds exactly 4096.
All inputs are finite; a program needn't handle non-finite values.
Results may differ from the reference program's by a relative error of at most 0.0003.
Values sent between devices are 32-bit elements; how exact they have to be, the bound alone decides.
A program may use at most 128 MiB of HBM per device.

```python
import jax
import jax.numpy as jnp
from jax import lax

COLS = 32
SPAN_LENGTH = 4096
STREAMS = 4
ROWS_DEV = 8192
N_ROWS = 32


def draw_events(key, part):
    noise_key, level_key = jax.random.split(jax.random.fold_in(key, 11), 2)
    shape = (STREAMS, COLS, ROWS_DEV * N_ROWS)
    noise = jax.random.truncated_normal(noise_key, -4.0, 4.0, shape, jnp.float32)
    levels = jax.random.uniform(level_key, (STREAMS, 1, N_ROWS), jnp.float32, -2.0, 2.0)
    levels = jnp.broadcast_to(levels, (STREAMS, COLS, N_ROWS))
    spread = jnp.repeat(levels, ROWS_DEV, axis=2, total_repeat_length=ROWS_DEV * N_ROWS)
    return (noise + spread).astype(jnp.float32)


def draw_keep_indicator(key, part):
    count_key, perm_key, forced_key = jax.random.split(jax.random.fold_in(key, 23), 3)
    draws = jax.random.randint(count_key, (STREAMS, N_ROWS, 2), 0, ROWS_DEV - SPAN_LENGTH + 1)
    keep = SPAN_LENGTH + jnp.min(draws, axis=2)
    forced = jax.random.randint(forced_key, (STREAMS, 1), 0, N_ROWS)
    keep = jnp.where(jnp.arange(N_ROWS)[None, :] == forced, SPAN_LENGTH, keep)
    keys = jax.random.split(perm_key, STREAMS * N_ROWS)
    perms = jax.vmap(lambda single: jax.random.permutation(single, ROWS_DEV))(keys)
    perms = perms.reshape(STREAMS, N_ROWS, ROWS_DEV)
    mask = (perms < keep[:, :, None]).astype(jnp.int32)
    return mask.reshape(STREAMS, N_ROWS * ROWS_DEV)


def setup_inputs(seed: int = 0) -> dict:
    streams_of = jax.random.split(jax.random.key(seed), 3)
    return {
        "events": draw_events(jax.random.fold_in(streams_of[2], 71), 0),
        "keep_indicator": draw_keep_indicator(jax.random.fold_in(streams_of[2], 71), 0),
    }


def single_table_input(pair):
    values, persisting_flags = pair
    feature_width = values.shape[0]
    total_rows = values.shape[1]
    retained_rows = values * persisting_flags[None, :].astype(jnp.float32)
    order = jnp.argsort(1 - persisting_flags, stable=True).astype(jnp.int32)
    packed_entries = jnp.take(retained_rows, order, axis=1)
    extended = jnp.concatenate([jnp.zeros((feature_width, SPAN_LENGTH), jnp.float32), packed_entries], axis=1)
    blocks = extended.reshape(feature_width, (total_rows + SPAN_LENGTH) // SPAN_LENGTH, SPAN_LENGTH)
    partial_sums = jnp.cumsum(blocks, axis=2)
    whole = partial_sums[:, :, -1]
    trailing = partial_sums[:, 1:, :] + (whole[:, :-1, None] - partial_sums[:, :-1, :])
    trailing = trailing.reshape(feature_width, total_rows)
    remaining_position = jnp.cumsum(persisting_flags).astype(jnp.int32)
    gather_slot = jnp.maximum(remaining_position - 1, 0).astype(jnp.int32)
    selected_entries = jnp.take(trailing, gather_slot, axis=1)
    lagging_mean = jnp.where(remaining_position[None, :] >= 1, selected_entries, jnp.float32(0.0)) / SPAN_LENGTH
    local = jnp.cumsum(retained_rows.reshape(feature_width, N_ROWS, ROWS_DEV), axis=2)
    ends = local[:, :, -1]
    starts = jnp.cumsum(ends, axis=1) - ends
    running = (local + starts[:, :, None]).reshape(feature_width, total_rows)
    visited_tally = jnp.maximum(remaining_position.astype(jnp.float32), 1.0)
    deviation = lagging_mean - running / visited_tally[None, :]
    return lagging_mean, deviation


def reference(events, keep_indicator):
    lagging_mean, deviation = lax.map(single_table_input, (events, keep_indicator))
    return (lagging_mean, deviation)
```

```python
import functools

import jax
import jax.numpy as jnp
from jax import lax
from jax.experimental import pallas as pl
from jax.experimental.pallas import tpu as pltpu
from jax.sharding import PartitionSpec as P

SPAN = 4096
LANES = 128
GROUP = 8
F32, BF16, I32 = jnp.float32, jnp.bfloat16, jnp.int32


def iota(shape, axis):
    return lax.broadcasted_iota(I32, shape, axis)


def lane_gather(values, index):
    return jnp.take_along_axis(values, index, axis=1, mode="promise_in_bounds")


def index_kernel(tiles, keep_ref, rank_ref, slot_ref, scalars_ref, flags):
    streams = keep_ref.shape[0]
    rows = streams * tiles
    for s in range(streams):
        for t in range(tiles):
            flags[s * tiles + t : s * tiles + t + 1, :] = keep_ref[s : s + 1, t * LANES : (t + 1) * LANES]
    kept = flags[...].astype(F32).astype(BF16)
    square = (LANES, LANES)
    upper = (iota(square, 0) <= iota(square, 1)).astype(F32).astype(BF16)
    ones = jnp.ones(square, BF16)
    within = jnp.dot(kept, upper, preferred_element_type=F32)
    counts = jnp.dot(kept, ones, preferred_element_type=F32).astype(BF16)
    grid = (rows, rows)
    same = (iota(grid, 0) // tiles) == (iota(grid, 1) // tiles)
    below = (same & (iota(grid, 1) < iota(grid, 0))).astype(F32).astype(BF16)
    above = (same & (iota(grid, 0) < iota(grid, 1))).astype(F32).astype(BF16)
    start = jnp.dot(below, counts, preferred_element_type=F32).astype(I32)
    within = within.astype(I32)
    rank_ref[...] = start + within
    lane = iota((rows, LANES), 1)
    wanted = ((lane - start - 1) & (LANES - 1)) + 1
    position = jnp.zeros((rows, LANES), I32)
    step = LANES // 2
    while step:
        seen = lane_gather(within, position + (step - 1))
        position = jnp.where(seen < wanted, position + step, position)
        step //= 2
    slot_ref[...] = position
    contract = (((1,), (1,)), ((), ()))
    first = (iota((8, LANES), 1) == 0).astype(F32).astype(BF16)
    count_row = lax.dot_general(jnp.ones((8, LANES), BF16), kept, contract, preferred_element_type=F32)
    first_row = lax.dot_general(first, kept, contract, preferred_element_type=F32)
    count_row = count_row.astype(BF16)
    start_row = jnp.dot(count_row, above, preferred_element_type=F32)
    total_row = jnp.dot(count_row, same.astype(F32).astype(BF16), preferred_element_type=F32)
    which = iota((8, rows), 0)
    row = jnp.where(which == 0, start_row, jnp.where(which == 1, total_row, start_row + first_row))
    scalars_ref[...] = row.astype(I32)


def pack_kernel(s, tiles, scalars_ref, events_ref, keep_ref, slot_ref, prefix_ref, table_ref, send_ref, total_ref):
    cols = events_ref.shape[1]
    lane = iota((cols, LANES), 1)
    shape = (2 * LANES, 2 * LANES)
    weights = (((iota(shape, 0) & (LANES - 1)) <= iota(shape, 1)).astype(F32)).astype(BF16)
    width = GROUP * LANES

    def group(g, carry):
        total, current = carry
        columns = pl.ds(pl.multiple_of(g * width, width), width)
        values = jnp.where(keep_ref[s : s + 1, columns] != 0, events_ref[0, :, columns], 0.0)
        high = values.astype(BF16)
        low = (values - high.astype(F32)).astype(BF16)
        left = jnp.concatenate([high[:, i * LANES : (i + 1) * LANES] for i in range(GROUP)], axis=0)
        right = jnp.concatenate([low[:, i * LANES : (i + 1) * LANES] for i in range(GROUP)], axis=0)
        sums = jnp.dot(jnp.concatenate([left, right], axis=1), weights, preferred_element_type=F32)
        for i in range(GROUP):
            t = g * GROUP + i
            piece = sums[i * cols : (i + 1) * cols]
            running = piece[:, :LANES] + total
            total = total + piece[:, LANES:]
            prefix_ref[t] = running
            order = jnp.broadcast_to(slot_ref[pl.ds(t, 1), :], (cols, LANES))
            packed = lane_gather(running, order)
            begin = scalars_ref[0, s * tiles + t] + 1
            block = begin // LANES
            merged = jnp.where(lane >= begin - block * LANES, packed, current)
            table_ref[block] = merged
            following = scalars_ref[0, s * tiles + jnp.minimum(t + 1, tiles - 1)] + 1
            current = jnp.where(following // LANES > block, packed, merged)
            table_ref[block + 1] = packed
        return total, current

    zeros = jnp.zeros((cols, LANES), F32)
    total, _ = lax.fori_loop(0, tiles // GROUP, group, (zeros, zeros))
    total_ref[...] = total
    base = scalars_ref[1, s * tiles] - SPAN
    origin = base // LANES
    offset = base - origin * LANES
    turn = (lane + offset) & (LANES - 1)

    def realign(g, carry):
        for i in range(GROUP):
            m = g * GROUP + i
            mixed = jnp.where(lane >= offset, table_ref[origin + m], table_ref[origin + m + 1])
            send_ref[m] = lane_gather(mixed, turn) - total
        return carry

    lax.fori_loop(0, SPAN // LANES // GROUP, realign, 0)


def spread_kernel(s, tiles, held, scalars_ref, earlier_ref, rank_ref, prefix_ref, before_ref, table_ref, tail_ref, *rest):
    mean_ref, deviation_ref, window, inverse, sems = rest[-5:]
    cols = prefix_ref.shape[1]
    back = SPAN // LANES
    copies = [
        pltpu.make_async_copy(tail_ref, window.at[pl.ds(0, back)], sems.at[0]),
        pltpu.make_async_copy(table_ref.at[pl.ds(0, held)], window.at[pl.ds(back, held)], sems.at[1]),
    ]
    for copy in copies:
        copy.start()
    visited = earlier_ref[s] + rank_ref[...].astype(F32)
    inverse[...] = 1.0 / jnp.maximum(visited, 1.0)
    for copy in copies:
        copy.wait()
    lane = iota((cols, LANES), 1)
    before = before_ref[0]

    def group(g, carry):
        for i in range(GROUP):
            t = g * GROUP + i
            begin = scalars_ref[2, s * tiles + t]
            block = begin // LANES
            mixed = jnp.where(lane >= begin - block * LANES, window[block], window[block + 1])
            order = jnp.broadcast_to(rank_ref[pl.ds(t, 1), :] & (LANES - 1), (cols, LANES))
            running = prefix_ref[t]
            mean = (running - lane_gather(mixed, order)) * (1.0 / SPAN)
            columns = pl.ds(pl.multiple_of(t * LANES, LANES), LANES)
            mean_ref[0, :, columns] = mean
            deviation_ref[0, :, columns] = mean - (running + before) * inverse[pl.ds(t, 1), :]
        return carry

    lax.fori_loop(0, tiles // GROUP, group, 0)


def vmem(*shape):
    return pl.BlockSpec(shape, lambda i: (0,) * len(shape))


def per_device(count, events, keep):
    streams, cols, rows = events.shape
    tiles = rows // LANES
    back = SPAN // LANES
    everything = streams * tiles
    held = (rows - SPAN) // LANES + 2
    smem = pl.BlockSpec(memory_space=pltpu.SMEM)
    anywhere = pl.BlockSpec(memory_space=pl.ANY)

    rank, slot, scalars = pl.pallas_call(
        functools.partial(index_kernel, tiles),
        out_shape=(
            jax.ShapeDtypeStruct((everything, LANES), I32),
            jax.ShapeDtypeStruct((everything, LANES), I32),
            jax.ShapeDtypeStruct((8, everything), I32),
        ),
        scratch_shapes=[pltpu.VMEM((everything, LANES), I32)],
        name="index",
    )(keep)

    prefixes, tables, totals, tails = [], [], [], []
    for s in range(streams):
        prefix, table, send, total = pl.pallas_call(
            functools.partial(pack_kernel, s, tiles),
            grid=(1,),
            in_specs=[
                smem,
                pl.BlockSpec((1, cols, rows), lambda i, s=s: (s, 0, 0)),
                vmem(streams, rows),
                pl.BlockSpec((tiles, LANES), lambda i, s=s: (s, 0)),
            ],
            out_specs=[
                vmem(tiles, cols, LANES),
                vmem(tiles + 2, cols, LANES),
                vmem(back, cols, LANES),
                vmem(cols, LANES),
            ],
            out_shape=[
                jax.ShapeDtypeStruct((tiles, cols, LANES), F32),
                jax.ShapeDtypeStruct((tiles + 2, cols, LANES), F32),
                jax.ShapeDtypeStruct((back, cols, LANES), F32),
                jax.ShapeDtypeStruct((cols, LANES), F32),
            ],
            cost_estimate=pl.CostEstimate(flops=10**8, bytes_accessed=8 * 2**20, transcendentals=0),
            name=f"pack{s}",
        )(scalars, events, keep, slot)
        tails.append(lax.ppermute(send, "rows", [(i, i + 1) for i in range(count - 1)]))
        prefixes.append(prefix)
        tables.append(table)
        totals.append(total)

    summary = jnp.concatenate(
        [jnp.stack([total[:, 0] for total in totals]), scalars[1, ::tiles].astype(F32)[:, None]], axis=1
    )
    gathered = lax.all_gather(summary, "rows", axis=0)
    earlier = jnp.arange(count, dtype=I32) < lax.axis_index("rows")
    before = jnp.sum(jnp.where(earlier[:, None, None], gathered, 0.0), axis=0)
    before_totals = jnp.broadcast_to(before[:, :cols, None], (streams, cols, LANES))
    before_counts = before[:, cols]

    outs = ()
    for s in range(streams):
        outs = pl.pallas_call(
            functools.partial(spread_kernel, s, tiles, held),
            grid=(1,),
            in_specs=[
                smem,
                smem,
                pl.BlockSpec((tiles, LANES), lambda i, s=s: (s, 0)),
                vmem(tiles, cols, LANES),
                pl.BlockSpec((1, cols, LANES), lambda i, s=s: (s, 0, 0)),
                anywhere,
                anywhere,
            ]
            + [anywhere] * len(outs),
            out_specs=[pl.BlockSpec((1, cols, rows), lambda i, s=s: (s, 0, 0))] * 2,
            out_shape=[jax.ShapeDtypeStruct(events.shape, F32)] * 2,
            scratch_shapes=[
                pltpu.VMEM((back + held, cols, LANES), F32),
                pltpu.VMEM((tiles, LANES), F32),
                pltpu.SemaphoreType.DMA((2,)),
            ],
            input_output_aliases={7: 0, 8: 1} if outs else {},
            cost_estimate=pl.CostEstimate(flops=10**8, bytes_accessed=8 * 2**20, transcendentals=0),
            name=f"spread{s}",
        )(scalars, before_counts, rank, prefixes[s], before_totals, tables[s], tails[s], *outs)
    return tuple(outs)


def solution(mesh):
    return jax.shard_map(
        functools.partial(per_device, mesh.shape["rows"]),
        mesh=mesh,
        in_specs=(P(None, None, "rows"), P(None, "rows")),
        out_specs=(P(None, None, "rows"), P(None, None, "rows")),
        check_vma=False,
    )
```

```python
import functools

import jax
import jax.numpy as jnp
from jax import lax
from jax.experimental import pallas as pl
from jax.experimental.pallas import tpu as pltpu
from jax.sharding import PartitionSpec as P

SPAN = 4096
LANES = 128
GROUP = 16
GRANT = 14 * 2**20
MESH = pl.DeviceIdType.MESH
F32, BF16, I32 = jnp.float32, jnp.bfloat16, jnp.int32


def iota(shape, axis):
    return lax.broadcasted_iota(I32, shape, axis)


def lane_gather(values, index):
    return jnp.take_along_axis(values, index, axis=1, mode="promise_in_bounds")


def index_kernel(tiles, keep_ref, rank_ref, slot_ref, scalars_ref, flags):
    streams = keep_ref.shape[0]
    rows = streams * tiles
    for s in range(streams):
        for t in range(tiles):
            flags[s * tiles + t : s * tiles + t + 1, :] = keep_ref[s : s + 1, t * LANES : (t + 1) * LANES]
    kept = flags[...].astype(F32).astype(BF16)
    square = (LANES, LANES)
    upper = (iota(square, 0) <= iota(square, 1)).astype(F32).astype(BF16)
    ones = jnp.ones(square, BF16)
    within = jnp.dot(kept, upper, preferred_element_type=F32)
    counts = jnp.dot(kept, ones, preferred_element_type=F32).astype(BF16)
    grid = (rows, rows)
    same = (iota(grid, 0) // tiles) == (iota(grid, 1) // tiles)
    below = (same & (iota(grid, 1) < iota(grid, 0))).astype(F32).astype(BF16)
    above = (same & (iota(grid, 0) < iota(grid, 1))).astype(F32).astype(BF16)
    start = jnp.dot(below, counts, preferred_element_type=F32).astype(I32)
    within = within.astype(I32)
    rank_ref[...] = start + within
    lane = iota((rows, LANES), 1)
    wanted = ((lane - start - 1) & (LANES - 1)) + 1
    position = jnp.zeros((rows, LANES), I32)
    step = LANES // 2
    while step:
        seen = lane_gather(within, position + (step - 1))
        position = jnp.where(seen < wanted, position + step, position)
        step //= 2
    slot_ref[...] = position
    contract = (((1,), (1,)), ((), ()))
    first = (iota((8, LANES), 1) == 0).astype(F32).astype(BF16)
    count_row = lax.dot_general(jnp.ones((8, LANES), BF16), kept, contract, preferred_element_type=F32)
    first_row = lax.dot_general(first, kept, contract, preferred_element_type=F32)
    count_row = count_row.astype(BF16)
    start_row = jnp.dot(count_row, above, preferred_element_type=F32)
    total_row = jnp.dot(count_row, same.astype(F32).astype(BF16), preferred_element_type=F32)
    which = iota((8, rows), 0)
    row = jnp.where(which == 0, start_row, jnp.where(which == 1, total_row, start_row + first_row))
    scalars_ref[...] = row.astype(I32)


def pack_kernel(s, tiles, group, scalars_ref, events_ref, keep_ref, slot_ref, *rest):
    prefix_ref, table_out, send_ref, total_ref, table_ref, current_ref, sem = rest[-7:]
    cols = events_ref.shape[1]
    held = table_out.shape[0]
    g = pl.program_id(0)
    lane = iota((cols, LANES), 1)
    shape = (2 * LANES, 2 * LANES)
    weights = (((iota(shape, 0) & (LANES - 1)) <= iota(shape, 1)).astype(F32)).astype(BF16)

    @pl.when(g == 0)
    def _():
        total_ref[...] = jnp.zeros((cols, LANES), F32)
        current_ref[...] = jnp.zeros((cols, LANES), F32)

    values = jnp.where(keep_ref[s : s + 1, :] != 0, events_ref[0], 0.0)
    high = values.astype(BF16)
    low = (values - high.astype(F32)).astype(BF16)
    left = jnp.concatenate([high[:, i * LANES : (i + 1) * LANES] for i in range(group)], axis=0)
    right = jnp.concatenate([low[:, i * LANES : (i + 1) * LANES] for i in range(group)], axis=0)
    sums = jnp.dot(jnp.concatenate([left, right], axis=1), weights, preferred_element_type=F32)
    total = total_ref[...]
    current = current_ref[...]
    for i in range(group):
        t = g * group + i
        piece = sums[i * cols : (i + 1) * cols]
        running = piece[:, :LANES] + total
        total = total + piece[:, LANES:]
        prefix_ref[i] = running
        order = jnp.broadcast_to(slot_ref[pl.ds(t, 1), :], (cols, LANES))
        packed = lane_gather(running, order)
        begin = scalars_ref[0, s * tiles + t] + 1
        block = begin // LANES
        merged = jnp.where(lane >= begin - block * LANES, packed, current)
        table_ref[block] = merged
        following = scalars_ref[0, s * tiles + jnp.minimum(t + 1, tiles - 1)] + 1
        current = jnp.where(following // LANES > block, packed, merged)
        if i == group - 1:
            table_ref[block + 1] = packed
    total_ref[...] = total
    current_ref[...] = current

    @pl.when(g == pl.num_programs(0) - 1)
    def _():
        copy = pltpu.make_async_copy(table_ref.at[pl.ds(0, held)], table_out, sem)
        copy.start()
        base = scalars_ref[1, s * tiles] - SPAN
        origin = base // LANES
        offset = base - origin * LANES
        turn = (lane + offset) & (LANES - 1)
        for m in range(SPAN // LANES):
            mixed = jnp.where(lane >= offset, table_ref[origin + m], table_ref[origin + m + 1])
            send_ref[m] = lane_gather(mixed, turn) - total
        copy.wait()


def exchange_kernel(count, streams, tiles, scalars_ref, *rest):
    total_refs, (before_ref, mine, slots, send_sems, recv_sems) = rest[:streams], rest[streams:]
    me = lax.axis_index("rows")
    barrier = pltpu.get_barrier_semaphore()

    def greet(j, carry):
        @pl.when(j < me)
        def _():
            pl.semaphore_signal(barrier, inc=1, device_id=(j,), device_id_type=MESH)

        return carry

    lax.fori_loop(0, count, greet, 0)
    width = mine.shape[1]
    cols = width // streams
    stacked = jnp.concatenate([ref[...] for ref in total_refs], axis=0)
    spread = jnp.full((8, LANES), 1.0 / LANES, F32)
    sums = lax.dot_general(
        spread, stacked, (((1,), (1,)), ((), ())), precision=lax.Precision.HIGHEST, preferred_element_type=F32
    )
    row, column = iota((8, width), 0), iota((8, width), 1)
    counts = jnp.zeros((8, width), F32)
    for s in range(streams):
        counts = jnp.where(column // cols == s, scalars_ref[1, s * tiles].astype(F32), counts)
    mine[...] = jnp.where(row == 0, sums, counts)
    before_ref[...] = jnp.zeros((8, width), F32)

    @pl.when(me < count - 1)
    def _():
        pl.semaphore_wait(barrier, count - 1 - me)

    def copy_to(j):
        return pltpu.make_async_remote_copy(
            src_ref=mine,
            dst_ref=slots.at[me],
            send_sem=send_sems.at[j],
            recv_sem=recv_sems.at[me],
            device_id=(j,),
            device_id_type=MESH,
        )

    def send(j, carry):
        @pl.when(j > me)
        def _():
            copy_to(j).start()

        return carry

    def receive(j, carry):
        @pl.when(j < me)
        def _():
            pltpu.make_async_remote_copy(
                src_ref=mine,
                dst_ref=slots.at[j],
                send_sem=send_sems.at[j],
                recv_sem=recv_sems.at[j],
                device_id=(j,),
                device_id_type=MESH,
            ).wait_recv()
            before_ref[...] += slots[j]

        return carry

    def finish(j, carry):
        @pl.when(j > me)
        def _():
            copy_to(j).wait_send()

        return carry

    lax.fori_loop(0, count, send, 0)
    lax.fori_loop(0, count, receive, 0)
    lax.fori_loop(0, count, finish, 0)


def spread_kernel(s, tiles, group, held, scalars_ref, before_ref, rank_ref, prefix_ref, table_ref, tail_ref, *rest):
    mean_ref, deviation_ref, window, inverse, offsets, sems = rest[-6:]
    cols = prefix_ref.shape[1]
    back = SPAN // LANES
    g = pl.program_id(0)

    @pl.when(g == 0)
    def _():
        copies = [
            pltpu.make_async_copy(tail_ref, window.at[pl.ds(0, back)], sems.at[0]),
            pltpu.make_async_copy(table_ref, window.at[pl.ds(back, held)], sems.at[1]),
        ]
        for copy in copies:
            copy.start()
        width = before_ref.shape[1]
        shape = (cols, width)
        mine = iota(shape, 1) == iota(shape, 0) + s * cols
        column = jnp.sum(jnp.where(mine, before_ref[0:1, :], 0.0), axis=1, keepdims=True)
        offsets[...] = jnp.broadcast_to(column, (cols, LANES))
        first = iota((1, width), 1) == s * cols
        earlier = jnp.sum(jnp.where(first, before_ref[1:2, :], 0.0), axis=1, keepdims=True)
        inverse[...] = 1.0 / jnp.maximum(earlier + rank_ref[...].astype(F32), 1.0)
        for copy in copies:
            copy.wait()

    lane = iota((cols, LANES), 1)
    before = offsets[...]
    for i in range(group):
        t = g * group + i
        begin = scalars_ref[2, s * tiles + t]
        block = begin // LANES
        mixed = jnp.where(lane >= begin - block * LANES, window[block], window[block + 1])
        order = jnp.broadcast_to(rank_ref[pl.ds(t, 1), :] & (LANES - 1), (cols, LANES))
        running = prefix_ref[i]
        mean = (running - lane_gather(mixed, order)) * (1.0 / SPAN)
        mean_ref[0, :, i * LANES : (i + 1) * LANES] = mean
        deviation_ref[0, :, i * LANES : (i + 1) * LANES] = mean - (running + before) * inverse[pl.ds(t, 1), :]


def whole(*shape):
    return pl.BlockSpec(shape, lambda i: (0,) * len(shape))


def per_device(count, events, keep):
    streams, cols, rows = events.shape
    tiles = rows // LANES
    back = SPAN // LANES
    everything = streams * tiles
    held = (rows - SPAN) // LANES + 2
    group = min(GROUP, tiles)
    steps = tiles // group
    smem = pl.BlockSpec(memory_space=pltpu.SMEM)
    anywhere = pl.BlockSpec(memory_space=pl.ANY)
    cost = pl.CostEstimate(flops=10**8, bytes_accessed=8 * 2**20, transcendentals=0)

    rank, slot, scalars = pl.pallas_call(
        functools.partial(index_kernel, tiles),
        out_shape=(
            jax.ShapeDtypeStruct((everything, LANES), I32),
            jax.ShapeDtypeStruct((everything, LANES), I32),
            jax.ShapeDtypeStruct((8, everything), I32),
        ),
        scratch_shapes=[pltpu.VMEM((everything, LANES), I32)],
        compiler_params=pltpu.CompilerParams(vmem_limit_bytes=GRANT),
        name="index",
    )(keep)

    prefixes, tables, totals, tails = [], [], [], []
    for s in range(streams):
        prefix, table, send, total = pl.pallas_call(
            functools.partial(pack_kernel, s, tiles, group),
            grid=(steps,),
            in_specs=[
                smem,
                pl.BlockSpec((1, cols, group * LANES), lambda i, s=s: (s, 0, i)),
                pl.BlockSpec((streams, group * LANES), lambda i: (0, i)),
                pl.BlockSpec((tiles, LANES), lambda i, s=s: (s, 0)),
            ]
            + [anywhere] * (s > 0),
            out_specs=[
                pl.BlockSpec((group, cols, LANES), lambda i: (i, 0, 0)),
                anywhere,
                whole(back, cols, LANES),
                whole(cols, LANES),
            ],
            out_shape=[
                jax.ShapeDtypeStruct((tiles, cols, LANES), F32),
                jax.ShapeDtypeStruct((held, cols, LANES), F32),
                jax.ShapeDtypeStruct((back, cols, LANES), F32),
                jax.ShapeDtypeStruct((cols, LANES), F32),
            ],
            scratch_shapes=[
                pltpu.VMEM((tiles + 2, cols, LANES), F32),
                pltpu.VMEM((cols, LANES), F32),
                pltpu.SemaphoreType.DMA,
            ],
            cost_estimate=cost,
            compiler_params=pltpu.CompilerParams(vmem_limit_bytes=GRANT),
            name=f"pack{s}",
        )(scalars, events, keep, slot, *totals[-1:])
        tails.append(lax.ppermute(send, "rows", [(i, i + 1) for i in range(count - 1)]))
        prefixes.append(prefix)
        tables.append(table)
        totals.append(total)

    width = streams * cols
    before = pl.pallas_call(
        functools.partial(exchange_kernel, count, streams, tiles),
        in_specs=[smem] + [pl.BlockSpec(memory_space=pltpu.VMEM)] * streams,
        out_specs=pl.BlockSpec(memory_space=pltpu.VMEM),
        out_shape=jax.ShapeDtypeStruct((8, width), F32),
        scratch_shapes=[
            pltpu.VMEM((8, width), F32),
            pltpu.VMEM((count, 8, width), F32),
            pltpu.SemaphoreType.DMA((count,)),
            pltpu.SemaphoreType.DMA((count,)),
        ],
        compiler_params=pltpu.CompilerParams(collective_id=0, has_side_effects=True, vmem_limit_bytes=GRANT),
        name="exchange",
    )(scalars, *totals)

    outs = ()
    for s in range(streams):
        outs = pl.pallas_call(
            functools.partial(spread_kernel, s, tiles, group, held),
            grid=(steps,),
            in_specs=[
                smem,
                whole(8, width),
                pl.BlockSpec((tiles, LANES), lambda i, s=s: (s, 0)),
                pl.BlockSpec((group, cols, LANES), lambda i: (i, 0, 0)),
                anywhere,
                anywhere,
            ]
            + [anywhere] * len(outs),
            out_specs=[pl.BlockSpec((1, cols, group * LANES), lambda i, s=s: (s, 0, i))] * 2,
            out_shape=[jax.ShapeDtypeStruct(events.shape, F32)] * 2,
            scratch_shapes=[
                pltpu.VMEM((back + held, cols, LANES), F32),
                pltpu.VMEM((tiles, LANES), F32),
                pltpu.VMEM((cols, LANES), F32),
                pltpu.SemaphoreType.DMA((2,)),
            ],
            input_output_aliases={6: 0, 7: 1} if outs else {},
            cost_estimate=cost,
            compiler_params=pltpu.CompilerParams(vmem_limit_bytes=GRANT),
            name=f"spread{s}",
        )(scalars, before, rank, prefixes[s], tables[s], tails[s], *outs)
    return tuple(outs)


def solution(mesh):
    return jax.shard_map(
        functools.partial(per_device, mesh.shape["rows"]),
        mesh=mesh,
        in_specs=(P(None, None, "rows"), P(None, "rows")),
        out_specs=(P(None, None, "rows"), P(None, None, "rows")),
        check_vma=False,
    )
```

```python
import functools

import jax
import jax.numpy as jnp
from jax import lax
from jax.experimental import pallas as pl
from jax.experimental.pallas import tpu as pltpu
from jax.sharding import PartitionSpec as P

SPAN = 4096
LANES = 128
GROUP = 16
GRANT = 20 * 2**20
HEAD_GRANT = 57 * 2**20
MESH = pl.DeviceIdType.MESH
F32, BF16, I32 = jnp.float32, jnp.bfloat16, jnp.int32


def iota(shape, axis):
    return lax.broadcasted_iota(I32, shape, axis)


def lane_gather(values, index):
    return jnp.take_along_axis(values, index, axis=1, mode="promise_in_bounds")


def index_kernel(tiles, keep_ref, rank_ref, slot_ref, scalars_ref, flags):
    streams = keep_ref.shape[0]
    rows = streams * tiles
    for s in range(streams):
        for t in range(tiles):
            flags[s * tiles + t : s * tiles + t + 1, :] = keep_ref[s : s + 1, t * LANES : (t + 1) * LANES]
    kept = flags[...].astype(F32).astype(BF16)
    square = (LANES, LANES)
    upper = (iota(square, 0) <= iota(square, 1)).astype(F32).astype(BF16)
    ones = jnp.ones(square, BF16)
    within = jnp.dot(kept, upper, preferred_element_type=F32)
    counts = jnp.dot(kept, ones, preferred_element_type=F32).astype(BF16)
    grid = (rows, rows)
    same = (iota(grid, 0) // tiles) == (iota(grid, 1) // tiles)
    below = (same & (iota(grid, 1) < iota(grid, 0))).astype(F32).astype(BF16)
    above = (same & (iota(grid, 0) < iota(grid, 1))).astype(F32).astype(BF16)
    start = jnp.dot(below, counts, preferred_element_type=F32).astype(I32)
    within = within.astype(I32)
    rank_ref[...] = start + within
    lane = iota((rows, LANES), 1)
    wanted = ((lane - start - 1) & (LANES - 1)) + 1
    position = jnp.zeros((rows, LANES), I32)
    step = LANES // 2
    while step:
        seen = lane_gather(within, position + (step - 1))
        position = jnp.where(seen < wanted, position + step, position)
        step //= 2
    slot_ref[...] = position
    contract = (((1,), (1,)), ((), ()))
    first = (iota((8, LANES), 1) == 0).astype(F32).astype(BF16)
    count_row = lax.dot_general(jnp.ones((8, LANES), BF16), kept, contract, preferred_element_type=F32)
    first_row = lax.dot_general(first, kept, contract, preferred_element_type=F32)
    count_row = count_row.astype(BF16)
    start_row = jnp.dot(count_row, above, preferred_element_type=F32)
    total_row = jnp.dot(count_row, same.astype(F32).astype(BF16), preferred_element_type=F32)
    which = iota((8, rows), 0)
    row = jnp.where(which == 0, start_row, jnp.where(which == 1, total_row, start_row + first_row))
    scalars_ref[...] = row.astype(I32)


def head_kernel(count, tiles, group, scalars_ref, events_ref, keep_ref, prefix_ref, before_ref, *scratch):
    held, mine, slots, load_sems, send_sems, recv_sems = scratch
    streams, cols, rows = held.shape
    width = streams * cols
    me = lax.axis_index("rows")
    barrier = pltpu.get_barrier_semaphore()

    loads = [pltpu.make_async_copy(events_ref.at[s], held.at[s], load_sems.at[s]) for s in range(streams)]
    for load in loads:
        load.start()

    def greet(j, carry):
        @pl.when(j < me)
        def _():
            pl.semaphore_signal(barrier, inc=1, device_id=(j,), device_id_type=MESH)

        return carry

    lax.fori_loop(0, count, greet, 0)
    span = group * LANES

    def masked(s, g):
        columns = pl.ds(pl.multiple_of(g * span, span), span)
        return jnp.where(keep_ref[s : s + 1, columns] != 0, held[s, :, columns], 0.0)

    totals = []
    for s in range(streams):
        loads[s].wait()

        def add(g, total, s=s):
            values = masked(s, g)
            parts = [values[:, i * LANES : (i + 1) * LANES] for i in range(group)]
            while len(parts) > 1:
                parts = [parts[i] + parts[i + 1] for i in range(0, len(parts), 2)]
            return total + parts[0]

        totals.append(lax.fori_loop(0, tiles // group, add, jnp.zeros((cols, LANES), F32)))
    sums = lax.dot_general(
        jnp.ones((8, LANES), F32),
        jnp.concatenate(totals, axis=0),
        (((1,), (1,)), ((), ())),
        precision=lax.Precision.HIGHEST,
        preferred_element_type=F32,
    )
    row, column = iota((8, width), 0), iota((8, width), 1)
    counts = jnp.zeros((8, width), F32)
    for s in range(streams):
        counts = jnp.where(column // cols == s, scalars_ref[1, s * tiles].astype(F32), counts)
    mine[...] = jnp.where(row == 0, sums, counts)
    before_ref[...] = jnp.zeros((8, width), F32)

    @pl.when(me < count - 1)
    def _():
        pl.semaphore_wait(barrier, count - 1 - me)

    def copy(j, sender):
        return pltpu.make_async_remote_copy(
            src_ref=mine,
            dst_ref=slots.at[sender],
            send_sem=send_sems.at[j],
            recv_sem=recv_sems.at[sender],
            device_id=(j,),
            device_id_type=MESH,
        )

    def send(j, carry):
        @pl.when(j > me)
        def _():
            copy(j, me).start()

        return carry

    lax.fori_loop(0, count, send, 0)

    shape = (2 * LANES, 2 * LANES)
    weights = (((iota(shape, 0) & (LANES - 1)) <= iota(shape, 1)).astype(F32)).astype(BF16)
    for s in range(streams):

        def accumulate(g, total, s=s):
            values = masked(s, g)
            high = values.astype(BF16)
            low = (values - high.astype(F32)).astype(BF16)
            left = jnp.concatenate([high[:, i * LANES : (i + 1) * LANES] for i in range(group)], axis=0)
            right = jnp.concatenate([low[:, i * LANES : (i + 1) * LANES] for i in range(group)], axis=0)
            out = jnp.dot(jnp.concatenate([left, right], axis=1), weights, preferred_element_type=F32)
            for i in range(group):
                piece = out[i * cols : (i + 1) * cols]
                prefix_ref[s * tiles + g * group + i] = piece[:, :LANES] + total
                total = total + piece[:, LANES:]
            return total

        lax.fori_loop(0, tiles // group, accumulate, jnp.zeros((cols, LANES), F32))

    def receive(j, carry):
        @pl.when(j < me)
        def _():
            copy(j, j).wait_recv()
            before_ref[...] += slots[j]

        return carry

    def finish(j, carry):
        @pl.when(j > me)
        def _():
            copy(j, me).wait_send()

        return carry

    lax.fori_loop(0, count, receive, 0)
    lax.fori_loop(0, count, finish, 0)


def pack_kernel(s, tiles, scalars_ref, prefix_ref, slot_ref, *rest):
    table_ref, send_ref = rest[-2:]
    cols = prefix_ref.shape[1]
    lane = iota((cols, LANES), 1)
    current = jnp.zeros((cols, LANES), F32)
    for t in range(tiles):
        order = jnp.broadcast_to(slot_ref[s * tiles + t : s * tiles + t + 1, :], (cols, LANES))
        packed = lane_gather(prefix_ref[s * tiles + t], order)
        begin = scalars_ref[0, s * tiles + t] + 1
        block = begin // LANES
        merged = jnp.where(lane >= begin - block * LANES, packed, current)
        table_ref[block] = merged
        if t == tiles - 1:
            table_ref[block + 1] = packed
        else:
            following = (scalars_ref[0, s * tiles + t + 1] + 1) // LANES
            current = jnp.where(following > block, packed, merged)
    last = prefix_ref[(s + 1) * tiles - 1]
    total = lane_gather(last, jnp.full((cols, LANES), LANES - 1, I32))
    base = scalars_ref[1, s * tiles] - SPAN
    origin = base // LANES
    offset = base - origin * LANES
    turn = (lane + offset) & (LANES - 1)
    below = table_ref[origin]
    for m in range(SPAN // LANES):
        above = table_ref[origin + m + 1]
        send_ref[m] = lane_gather(jnp.where(lane >= offset, below, above), turn) - total
        below = above


def spread_kernel(s, tiles, group, scalars_ref, before_ref, rank_ref, prefix_ref, table_ref, tail_ref, *rest):
    mean_ref, deviation_ref, means, deviations, inverse, sems = rest[-6:]
    cols = prefix_ref.shape[1]
    back = SPAN // LANES
    width = before_ref.shape[1]
    mine = iota((cols, width), 1) == iota((cols, width), 0) + s * cols
    column = jnp.sum(jnp.where(mine, before_ref[0:1, :], 0.0), axis=1, keepdims=True)
    before = jnp.broadcast_to(column, (cols, LANES))
    first = iota((1, width), 1) == s * cols
    earlier = jnp.sum(jnp.where(first, before_ref[1:2, :], 0.0), axis=1, keepdims=True)
    ranks = rank_ref[s * tiles : (s + 1) * tiles, :]
    inverse[...] = 1.0 / jnp.maximum(earlier + ranks.astype(F32), 1.0)
    lane = iota((cols, LANES), 1)

    def fetch(block):
        old = tail_ref[jnp.minimum(block, back - 1)]
        new = table_ref[jnp.maximum(block - back, 0)]
        return jnp.where(block < back, old, new)

    copies = []
    for g in range(tiles // group):
        for i in range(group):
            t = g * group + i
            begin = scalars_ref[2, s * tiles + t]
            block = begin // LANES
            mixed = jnp.where(lane >= begin - block * LANES, fetch(block), fetch(block + 1))
            order = jnp.broadcast_to(rank_ref[s * tiles + t : s * tiles + t + 1, :] & (LANES - 1), (cols, LANES))
            running = prefix_ref[s * tiles + t]
            mean = (running - lane_gather(mixed, order)) * (1.0 / SPAN)
            columns = slice(t * LANES, (t + 1) * LANES)
            means[:, columns] = mean
            deviations[:, columns] = mean - (running + before) * inverse[t : t + 1, :]
        part = pl.ds(g * group * LANES, group * LANES)
        for k, (source, target) in enumerate(((means, mean_ref), (deviations, deviation_ref))):
            copy = pltpu.make_async_copy(source.at[:, part], target.at[s, :, part], sems.at[k, g])
            copy.start()
            copies.append(copy)
    for copy in copies:
        copy.wait()


def per_device(count, events, keep):
    streams, cols, rows = events.shape
    tiles = rows // LANES
    back = SPAN // LANES
    everything = streams * tiles
    width = streams * cols
    group = min(GROUP, tiles)
    smem = pl.BlockSpec(memory_space=pltpu.SMEM)
    vmem = pl.BlockSpec(memory_space=pltpu.VMEM)
    anywhere = pl.BlockSpec(memory_space=pl.ANY)
    cost = pl.CostEstimate(flops=10**8, bytes_accessed=8 * 2**20, transcendentals=0)
    params = pltpu.CompilerParams(vmem_limit_bytes=GRANT)

    rank, slot, scalars = pl.pallas_call(
        functools.partial(index_kernel, tiles),
        out_shape=(
            jax.ShapeDtypeStruct((everything, LANES), I32),
            jax.ShapeDtypeStruct((everything, LANES), I32),
            jax.ShapeDtypeStruct((8, everything), I32),
        ),
        scratch_shapes=[pltpu.VMEM((everything, LANES), I32)],
        compiler_params=params,
        name="index",
    )(keep)

    prefix, before = pl.pallas_call(
        functools.partial(head_kernel, count, tiles, group),
        in_specs=[smem, anywhere, vmem],
        out_specs=[vmem, vmem],
        out_shape=[
            jax.ShapeDtypeStruct((everything, cols, LANES), F32),
            jax.ShapeDtypeStruct((8, width), F32),
        ],
        scratch_shapes=[
            pltpu.VMEM((streams, cols, rows), F32),
            pltpu.VMEM((8, width), F32),
            pltpu.VMEM((count, 8, width), F32),
            pltpu.SemaphoreType.DMA((streams,)),
            pltpu.SemaphoreType.DMA((count,)),
            pltpu.SemaphoreType.DMA((count,)),
        ],
        compiler_params=pltpu.CompilerParams(collective_id=0, has_side_effects=True, vmem_limit_bytes=HEAD_GRANT),
        name="head",
    )(scalars, events, keep)

    tables, tails, sent = [], [], []
    for s in range(streams):
        table, send = pl.pallas_call(
            functools.partial(pack_kernel, s, tiles),
            in_specs=[smem, vmem, vmem] + [anywhere] * (s > 0),
            out_specs=[vmem, vmem],
            out_shape=[
                jax.ShapeDtypeStruct((tiles + 2, cols, LANES), F32),
                jax.ShapeDtypeStruct((back, cols, LANES), F32),
            ],
            cost_estimate=cost,
            compiler_params=params,
            name=f"pack{s}",
        )(scalars, prefix, slot, *tables[-1:])
        tails.append(lax.ppermute(send, "rows", [(i, i + 1) for i in range(count - 1)]))
        tables.append(table)

    outs = ()
    for s in range(streams):
        outs = pl.pallas_call(
            functools.partial(spread_kernel, s, tiles, group),
            in_specs=[smem] + [vmem] * 5 + [anywhere] * len(outs),
            out_specs=[anywhere] * 2,
            out_shape=[jax.ShapeDtypeStruct(events.shape, F32)] * 2,
            scratch_shapes=[
                pltpu.VMEM((cols, rows), F32),
                pltpu.VMEM((cols, rows), F32),
                pltpu.VMEM((tiles, LANES), F32),
                pltpu.SemaphoreType.DMA((2, tiles // group)),
            ],
            input_output_aliases={6: 0, 7: 1} if outs else {},
            cost_estimate=cost,
            compiler_params=params,
            name=f"spread{s}",
        )(scalars, before, rank, prefix, tables[s], tails[s], *outs)
    return tuple(outs)


def solution(mesh):
    return jax.shard_map(
        functools.partial(per_device, mesh.shape["rows"]),
        mesh=mesh,
        in_specs=(P(None, None, "rows"), P(None, "rows")),
        out_specs=(P(None, None, "rows"), P(None, None, "rows")),
        check_vma=False,
    )
```

```python
import functools

import jax
import jax.numpy as jnp
from jax import lax
from jax.experimental import pallas as pl
from jax.experimental.pallas import tpu as pltpu
from jax.sharding import PartitionSpec as P

SPAN = 4096
LANES = 128
GROUP = 16
GRANT = 8 * 2**20
GATHERED = 2**20
F32, BF16, I32 = jnp.float32, jnp.bfloat16, jnp.int32


def iota(shape, axis):
    return lax.broadcasted_iota(I32, shape, axis)


def lane_gather(values, index):
    return jnp.take_along_axis(values, index, axis=1, mode="promise_in_bounds")


def prepare_kernel(tiles, events_hbm, keep_hbm, events_ref, keep_ref, rank_ref, slot_ref, scalars_ref, mine_ref, flags, sems):
    streams, cols, _ = events_ref.shape
    rows = streams * tiles
    flag_load = pltpu.make_async_copy(keep_hbm, keep_ref, sems.at[streams])
    flag_load.start()
    loads = [pltpu.make_async_copy(events_hbm.at[s], events_ref.at[s], sems.at[s]) for s in range(streams)]
    for load in loads:
        load.start()
    flag_load.wait()
    for s in range(streams):
        for t in range(tiles):
            flags[s * tiles + t : s * tiles + t + 1, :] = keep_ref[s : s + 1, t * LANES : (t + 1) * LANES]
    kept = flags[...].astype(F32).astype(BF16)
    square = (LANES, LANES)
    upper = (iota(square, 0) <= iota(square, 1)).astype(F32).astype(BF16)
    ones = jnp.ones(square, BF16)
    within = jnp.dot(kept, upper, preferred_element_type=F32)
    counts = jnp.dot(kept, ones, preferred_element_type=F32).astype(BF16)
    grid = (rows, rows)
    same = (iota(grid, 0) // tiles) == (iota(grid, 1) // tiles)
    below = (same & (iota(grid, 1) < iota(grid, 0))).astype(F32).astype(BF16)
    above = (same & (iota(grid, 0) < iota(grid, 1))).astype(F32).astype(BF16)
    start = jnp.dot(below, counts, preferred_element_type=F32).astype(I32)
    within = within.astype(I32)
    rank_ref[...] = start + within
    lane = iota((rows, LANES), 1)
    wanted = ((lane - start - 1) & (LANES - 1)) + 1
    position = jnp.zeros((rows, LANES), I32)
    step = LANES // 2
    while step:
        seen = lane_gather(within, position + (step - 1))
        position = jnp.where(seen < wanted, position + step, position)
        step //= 2
    slot_ref[...] = position
    contract = (((1,), (1,)), ((), ()))
    first = (iota((8, LANES), 1) == 0).astype(F32).astype(BF16)
    count_row = lax.dot_general(jnp.ones((8, LANES), BF16), kept, contract, preferred_element_type=F32)
    first_row = lax.dot_general(first, kept, contract, preferred_element_type=F32)
    count_row = count_row.astype(BF16)
    start_row = jnp.dot(count_row, above, preferred_element_type=F32)
    total_row = jnp.dot(count_row, same.astype(F32).astype(BF16), preferred_element_type=F32)
    which = iota((8, rows), 0)
    row = jnp.where(which == 0, start_row, jnp.where(which == 1, total_row, start_row + first_row))
    scalars_ref[...] = row.astype(I32)
    group = 8
    span = group * LANES
    totals = []
    for s in range(streams):
        loads[s].wait()

        def add(g, total, s=s):
            columns = pl.ds(pl.multiple_of(g * span, span), span)
            values = jnp.where(keep_ref[s : s + 1, columns] != 0, events_ref[s, :, columns], 0.0)
            parts = [values[:, i * LANES : (i + 1) * LANES] for i in range(group)]
            while len(parts) > 1:
                parts = [parts[i] + parts[i + 1] for i in range(0, len(parts), 2)]
            return total + parts[0]

        totals.append(lax.fori_loop(0, tiles // group, add, jnp.zeros((cols, LANES), F32), unroll=True))
    sums = lax.dot_general(
        jnp.ones((8, LANES), F32),
        jnp.concatenate(totals, axis=0),
        contract,
        precision=lax.Precision.HIGHEST,
        preferred_element_type=F32,
    )
    width = streams * cols
    line, column = iota((8, width), 0), iota((8, width), 1)
    tallies = jnp.zeros((8, width), F32)
    for s in range(streams):
        tallies = jnp.where(column // cols == s, total_row[:, s * tiles : s * tiles + 1], tallies)
    mine_ref[...] = jnp.zeros(mine_ref.shape, F32)
    mine_ref[0:8, :] = jnp.where(line == 0, sums, tallies)


def pack_kernel(s, tiles, group, scalars_ref, events_ref, keep_ref, slot_ref, *rest):
    prefix_ref, table_ref, send_ref = rest[-3:]
    cols = prefix_ref.shape[1]
    lane = iota((cols, LANES), 1)
    shape = (2 * LANES, 2 * LANES)
    weights = (((iota(shape, 0) & (LANES - 1)) <= iota(shape, 1)).astype(F32)).astype(BF16)
    total = jnp.zeros((cols, LANES), F32)
    current = jnp.zeros((cols, LANES), F32)
    for g in range(tiles // group):
        left, right = [], []
        for i in range(group):
            columns = slice((g * group + i) * LANES, (g * group + i + 1) * LANES)
            values = jnp.where(keep_ref[s : s + 1, columns] != 0, events_ref[s, :, columns], 0.0)
            high = values.astype(BF16)
            left.append(high)
            right.append((values - high.astype(F32)).astype(BF16))
        pair = jnp.concatenate([jnp.concatenate(left, axis=0), jnp.concatenate(right, axis=0)], axis=1)
        sums = jnp.dot(pair, weights, preferred_element_type=F32)
        for i in range(group):
            t = g * group + i
            piece = sums[i * cols : (i + 1) * cols]
            running = piece[:, :LANES] + total
            total = total + piece[:, LANES:]
            prefix_ref[t] = running
            order = jnp.broadcast_to(slot_ref[s * tiles + t : s * tiles + t + 1, :], (cols, LANES))
            packed = lane_gather(running, order)
            begin = scalars_ref[0, s * tiles + t] + 1
            block = begin // LANES
            merged = jnp.where(lane >= begin - block * LANES, packed, current)
            table_ref[block] = merged
            if t == tiles - 1:
                table_ref[block + 1] = packed
            else:
                following = (scalars_ref[0, s * tiles + t + 1] + 1) // LANES
                current = jnp.where(following > block, packed, merged)
    base = scalars_ref[1, s * tiles] - SPAN
    origin = base // LANES
    offset = base - origin * LANES
    turn = (lane + offset) & (LANES - 1)
    below = table_ref[origin]
    for m in range(SPAN // LANES):
        above = table_ref[origin + m + 1]
        send_ref[m] = lane_gather(jnp.where(lane >= offset, below, above), turn) - total
        below = above


def spread_kernel(s, tiles, group, scalars_ref, before_ref, rank_ref, prefix_ref, table_ref, tail_ref, *rest):
    mean_ref, deviation_ref, means, deviations, inverse, sems = rest[-6:]
    cols = prefix_ref.shape[1]
    back = SPAN // LANES
    width = before_ref.shape[1]
    mine = iota((cols, width), 1) == iota((cols, width), 0) + s * cols
    column = jnp.sum(jnp.where(mine, before_ref[0:1, :], 0.0), axis=1, keepdims=True)
    before = jnp.broadcast_to(column, (cols, LANES))
    first = iota((1, width), 1) == s * cols
    earlier = jnp.sum(jnp.where(first, before_ref[1:2, :], 0.0), axis=1, keepdims=True)
    ranks = rank_ref[s * tiles : (s + 1) * tiles, :]
    inverse[...] = 1.0 / jnp.maximum(earlier + ranks.astype(F32), 1.0)
    lane = iota((cols, LANES), 1)

    def fetch(block):
        old = tail_ref[jnp.minimum(block, back - 1)]
        new = table_ref[jnp.maximum(block - back, 0)]
        return jnp.where(block < back, old, new)

    copies = []
    for g in range(tiles // group):
        for i in range(group):
            t = g * group + i
            begin = scalars_ref[2, s * tiles + t]
            block = begin // LANES
            mixed = jnp.where(lane >= begin - block * LANES, fetch(block), fetch(block + 1))
            order = jnp.broadcast_to(rank_ref[s * tiles + t : s * tiles + t + 1, :] & (LANES - 1), (cols, LANES))
            running = prefix_ref[t]
            mean = (running - lane_gather(mixed, order)) * (1.0 / SPAN)
            columns = slice(t * LANES, (t + 1) * LANES)
            means[:, columns] = mean
            deviations[:, columns] = mean - (running + before) * inverse[t : t + 1, :]
        part = pl.ds(g * group * LANES, group * LANES)
        for k, (source, target) in enumerate(((means, mean_ref), (deviations, deviation_ref))):
            copy = pltpu.make_async_copy(source.at[:, part], target.at[s, :, part], sems.at[k, g])
            copy.start()
            copies.append(copy)
    for copy in copies:
        copy.wait()


def per_device(count, events, keep):
    streams, cols, rows = events.shape
    tiles = rows // LANES
    back = SPAN // LANES
    everything = streams * tiles
    width = streams * cols
    group = min(GROUP, tiles)
    smem = pl.BlockSpec(memory_space=pltpu.SMEM)
    vmem = pl.BlockSpec(memory_space=pltpu.VMEM)
    hbm = pl.BlockSpec(memory_space=pltpu.HBM)
    anywhere = pl.BlockSpec(memory_space=pl.ANY)
    cost = pl.CostEstimate(flops=10**8, bytes_accessed=8 * 2**20, transcendentals=0)
    params = pltpu.CompilerParams(vmem_limit_bytes=GRANT)
    lines = 8 * pl.cdiv(GATHERED, count * width * 4 * 8)

    events, keep, rank, slot, scalars, mine = pl.pallas_call(
        functools.partial(prepare_kernel, tiles),
        in_specs=[hbm, hbm],
        out_specs=[vmem] * 6,
        out_shape=(
            jax.ShapeDtypeStruct(events.shape, F32),
            jax.ShapeDtypeStruct(keep.shape, I32),
            jax.ShapeDtypeStruct((everything, LANES), I32),
            jax.ShapeDtypeStruct((everything, LANES), I32),
            jax.ShapeDtypeStruct((8, everything), I32),
            jax.ShapeDtypeStruct((lines, width), F32),
        ),
        scratch_shapes=[pltpu.VMEM((everything, LANES), I32), pltpu.SemaphoreType.DMA((streams + 1,))],
        compiler_params=params,
        name="prepare",
    )(events, keep)
    gathered = lax.all_gather(mine, "rows", axis=0, tiled=True).reshape(count, lines, width)[:, :8]
    earlier = jnp.arange(count, dtype=I32) < lax.axis_index("rows")
    before = jnp.sum(jnp.where(earlier[:, None, None], gathered, 0.0), axis=0)

    prefixes, tables, tails = [], [], []
    for s in range(streams):
        prefix, table, send = pl.pallas_call(
            functools.partial(pack_kernel, s, tiles, group),
            in_specs=[smem, vmem, vmem, vmem] + [anywhere] * (s > 0),
            out_specs=[vmem, vmem, vmem],
            out_shape=[
                jax.ShapeDtypeStruct((tiles, cols, LANES), F32),
                jax.ShapeDtypeStruct((tiles + 2, cols, LANES), F32),
                jax.ShapeDtypeStruct((back, cols, LANES), F32),
            ],
            cost_estimate=cost,
            compiler_params=params,
            name=f"pack{s}",
        )(scalars, events, keep, slot, *tables[-1:])
        tails.append(lax.ppermute(send, "rows", [(i, i + 1) for i in range(count - 1)]))
        prefixes.append(prefix)
        tables.append(table)

    outs = ()
    shape = (streams, cols, rows)
    for s in range(streams):
        outs = pl.pallas_call(
            functools.partial(spread_kernel, s, tiles, group),
            in_specs=[smem] + [vmem] * 5 + [anywhere] * len(outs),
            out_specs=[anywhere] * 2,
            out_shape=[jax.ShapeDtypeStruct(shape, F32)] * 2,
            scratch_shapes=[
                pltpu.VMEM((cols, rows), F32),
                pltpu.VMEM((cols, rows), F32),
                pltpu.VMEM((tiles, LANES), F32),
                pltpu.SemaphoreType.DMA((2, tiles // group)),
            ],
            input_output_aliases={6: 0, 7: 1} if outs else {},
            cost_estimate=cost,
            compiler_params=params,
            name=f"spread{s}",
        )(scalars, before, rank, prefixes[s], tables[s], tails[s], *outs)
    return tuple(outs)


def solution(mesh):
    return jax.shard_map(
        functools.partial(per_device, mesh.shape["rows"]),
        mesh=mesh,
        in_specs=(P(None, None, "rows"), P(None, "rows")),
        out_specs=(P(None, None, "rows"), P(None, None, "rows")),
        check_vma=False,
    )
```

```python
import functools

import jax
import jax.numpy as jnp
from jax import lax
from jax.experimental import pallas as pl
from jax.experimental.pallas import tpu as pltpu
from jax.sharding import PartitionSpec as P

SPAN = 4096
LANES = 128
GROUP = 16
GRANT = 16 * 2**20
MESH = pl.DeviceIdType.MESH
F32, BF16, I32 = jnp.float32, jnp.bfloat16, jnp.int32


def iota(shape, axis):
    return lax.broadcasted_iota(I32, shape, axis)


def lane_gather(values, index):
    return jnp.take_along_axis(values, index, axis=1, mode="promise_in_bounds")


def index_kernel(tiles, keep_ref, rank_ref, slot_ref, scalars_ref, flags):
    streams = keep_ref.shape[0]
    rows = streams * tiles
    for s in range(streams):
        for t in range(tiles):
            flags[s * tiles + t : s * tiles + t + 1, :] = keep_ref[s : s + 1, t * LANES : (t + 1) * LANES]
    kept = flags[...].astype(F32).astype(BF16)
    square = (LANES, LANES)
    upper = (iota(square, 0) <= iota(square, 1)).astype(F32).astype(BF16)
    ones = jnp.ones(square, BF16)
    within = jnp.dot(kept, upper, preferred_element_type=F32)
    counts = jnp.dot(kept, ones, preferred_element_type=F32).astype(BF16)
    grid = (rows, rows)
    same = (iota(grid, 0) // tiles) == (iota(grid, 1) // tiles)
    below = (same & (iota(grid, 1) < iota(grid, 0))).astype(F32).astype(BF16)
    above = (same & (iota(grid, 0) < iota(grid, 1))).astype(F32).astype(BF16)
    start = jnp.dot(below, counts, preferred_element_type=F32).astype(I32)
    within = within.astype(I32)
    rank_ref[...] = start + within
    lane = iota((rows, LANES), 1)
    wanted = ((lane - start - 1) & (LANES - 1)) + 1
    position = jnp.zeros((rows, LANES), I32)
    step = LANES // 2
    while step:
        seen = lane_gather(within, position + (step - 1))
        position = jnp.where(seen < wanted, position + step, position)
        step //= 2
    slot_ref[...] = position
    contract = (((1,), (1,)), ((), ()))
    first = (iota((8, LANES), 1) == 0).astype(F32).astype(BF16)
    count_row = lax.dot_general(jnp.ones((8, LANES), BF16), kept, contract, preferred_element_type=F32)
    first_row = lax.dot_general(first, kept, contract, preferred_element_type=F32)
    count_row = count_row.astype(BF16)
    start_row = jnp.dot(count_row, above, preferred_element_type=F32)
    total_row = jnp.dot(count_row, same.astype(F32).astype(BF16), preferred_element_type=F32)
    which = iota((8, rows), 0)
    row = jnp.where(which == 0, start_row, jnp.where(which == 1, total_row, start_row + first_row))
    scalars_ref[...] = row.astype(I32)


def head_kernel(count, tiles, group, scalars_ref, events_ref, keep_ref, prefix_ref, before_ref, *scratch):
    mine, slots, send_sems, recv_sems = scratch
    streams, cols, rows = events_ref.shape
    width = streams * cols
    me = lax.axis_index("rows")
    barrier = pltpu.get_barrier_semaphore()

    def greet(j, carry):
        @pl.when(j < me)
        def _():
            pl.semaphore_signal(barrier, inc=1, device_id=(j,), device_id_type=MESH)

        return carry

    lax.fori_loop(0, count, greet, 0)
    span = group * LANES

    def masked(s, g):
        columns = pl.ds(pl.multiple_of(g * span, span), span)
        return jnp.where(keep_ref[s : s + 1, columns] != 0, events_ref[s, :, columns], 0.0)

    totals = []
    for s in range(streams):

        def add(g, total, s=s):
            values = masked(s, g)
            parts = [values[:, i * LANES : (i + 1) * LANES] for i in range(group)]
            while len(parts) > 1:
                parts = [parts[i] + parts[i + 1] for i in range(0, len(parts), 2)]
            return total + parts[0]

        totals.append(lax.fori_loop(0, tiles // group, add, jnp.zeros((cols, LANES), F32), unroll=True))
    sums = lax.dot_general(
        jnp.ones((8, LANES), F32),
        jnp.concatenate(totals, axis=0),
        (((1,), (1,)), ((), ())),
        precision=lax.Precision.HIGHEST,
        preferred_element_type=F32,
    )
    row, column = iota((8, width), 0), iota((8, width), 1)
    counts = jnp.zeros((8, width), F32)
    for s in range(streams):
        counts = jnp.where(column // cols == s, scalars_ref[1, s * tiles].astype(F32), counts)
    mine[...] = jnp.where(row == 0, sums, counts)
    before_ref[...] = jnp.zeros((8, width), F32)

    @pl.when(me < count - 1)
    def _():
        pl.semaphore_wait(barrier, count - 1 - me)

    def copy(j, sender):
        return pltpu.make_async_remote_copy(
            src_ref=mine,
            dst_ref=slots.at[sender],
            send_sem=send_sems.at[j],
            recv_sem=recv_sems.at[sender],
            device_id=(j,),
            device_id_type=MESH,
        )

    def send(j, carry):
        @pl.when(j > me)
        def _():
            copy(j, me).start()

        return carry

    lax.fori_loop(0, count, send, 0)

    shape = (2 * LANES, 2 * LANES)
    weights = (((iota(shape, 0) & (LANES - 1)) <= iota(shape, 1)).astype(F32)).astype(BF16)
    for s in range(streams):

        def accumulate(g, total, s=s):
            values = masked(s, g)
            high = values.astype(BF16)
            low = (values - high.astype(F32)).astype(BF16)
            left = jnp.concatenate([high[:, i * LANES : (i + 1) * LANES] for i in range(group)], axis=0)
            right = jnp.concatenate([low[:, i * LANES : (i + 1) * LANES] for i in range(group)], axis=0)
            out = jnp.dot(jnp.concatenate([left, right], axis=1), weights, preferred_element_type=F32)
            for i in range(group):
                piece = out[i * cols : (i + 1) * cols]
                prefix_ref[s * tiles + g * group + i] = piece[:, :LANES] + total
                total = total + piece[:, LANES:]
            return total

        lax.fori_loop(0, tiles // group, accumulate, jnp.zeros((cols, LANES), F32))

    def receive(j, carry):
        @pl.when(j < me)
        def _():
            copy(j, j).wait_recv()
            before_ref[...] += slots[j]

        return carry

    def finish(j, carry):
        @pl.when(j > me)
        def _():
            copy(j, me).wait_send()

        return carry

    lax.fori_loop(0, count, receive, 0)
    lax.fori_loop(0, count, finish, 0)


def pack_kernel(s, tiles, scalars_ref, prefix_ref, slot_ref, *rest):
    table_ref, send_ref = rest[-2:]
    cols = prefix_ref.shape[1]
    lane = iota((cols, LANES), 1)
    current = jnp.zeros((cols, LANES), F32)
    for t in range(tiles):
        order = jnp.broadcast_to(slot_ref[s * tiles + t : s * tiles + t + 1, :], (cols, LANES))
        packed = lane_gather(prefix_ref[s * tiles + t], order)
        begin = scalars_ref[0, s * tiles + t] + 1
        block = begin // LANES
        merged = jnp.where(lane >= begin - block * LANES, packed, current)
        table_ref[block] = merged
        if t == tiles - 1:
            table_ref[block + 1] = packed
        else:
            following = (scalars_ref[0, s * tiles + t + 1] + 1) // LANES
            current = jnp.where(following > block, packed, merged)
    last = prefix_ref[(s + 1) * tiles - 1]
    total = lane_gather(last, jnp.full((cols, LANES), LANES - 1, I32))
    base = scalars_ref[1, s * tiles] - SPAN
    origin = base // LANES
    offset = base - origin * LANES
    turn = (lane + offset) & (LANES - 1)
    below = table_ref[origin]
    for m in range(SPAN // LANES):
        above = table_ref[origin + m + 1]
        send_ref[m] = lane_gather(jnp.where(lane >= offset, below, above), turn) - total
        below = above


def spread_kernel(s, tiles, group, scalars_ref, before_ref, rank_ref, prefix_ref, table_ref, tail_ref, *rest):
    mean_ref, deviation_ref, means, deviations, inverse, sems = rest[-6:]
    cols = prefix_ref.shape[1]
    back = SPAN // LANES
    width = before_ref.shape[1]
    mine = iota((cols, width), 1) == iota((cols, width), 0) + s * cols
    column = jnp.sum(jnp.where(mine, before_ref[0:1, :], 0.0), axis=1, keepdims=True)
    before = jnp.broadcast_to(column, (cols, LANES))
    first = iota((1, width), 1) == s * cols
    earlier = jnp.sum(jnp.where(first, before_ref[1:2, :], 0.0), axis=1, keepdims=True)
    ranks = rank_ref[s * tiles : (s + 1) * tiles, :]
    inverse[...] = 1.0 / jnp.maximum(earlier + ranks.astype(F32), 1.0)
    lane = iota((cols, LANES), 1)

    def fetch(block):
        old = tail_ref[jnp.minimum(block, back - 1)]
        new = table_ref[jnp.maximum(block - back, 0)]
        return jnp.where(block < back, old, new)

    copies = []
    for g in range(tiles // group):
        for i in range(group):
            t = g * group + i
            begin = scalars_ref[2, s * tiles + t]
            block = begin // LANES
            mixed = jnp.where(lane >= begin - block * LANES, fetch(block), fetch(block + 1))
            order = jnp.broadcast_to(rank_ref[s * tiles + t : s * tiles + t + 1, :] & (LANES - 1), (cols, LANES))
            running = prefix_ref[s * tiles + t]
            mean = (running - lane_gather(mixed, order)) * (1.0 / SPAN)
            columns = slice(t * LANES, (t + 1) * LANES)
            means[:, columns] = mean
            deviations[:, columns] = mean - (running + before) * inverse[t : t + 1, :]
        part = pl.ds(g * group * LANES, group * LANES)
        for k, (source, target) in enumerate(((means, mean_ref), (deviations, deviation_ref))):
            copy = pltpu.make_async_copy(source.at[:, part], target.at[s, :, part], sems.at[k, g])
            copy.start()
            copies.append(copy)
    for copy in copies:
        copy.wait()


def per_device(count, events, keep):
    streams, cols, rows = events.shape
    tiles = rows // LANES
    back = SPAN // LANES
    everything = streams * tiles
    width = streams * cols
    group = min(GROUP, tiles)
    smem = pl.BlockSpec(memory_space=pltpu.SMEM)
    vmem = pl.BlockSpec(memory_space=pltpu.VMEM)
    anywhere = pl.BlockSpec(memory_space=pl.ANY)
    cost = pl.CostEstimate(flops=10**9, bytes_accessed=8 * 2**20, transcendentals=0)
    params = pltpu.CompilerParams(vmem_limit_bytes=GRANT)

    rank, slot, scalars = pl.pallas_call(
        functools.partial(index_kernel, tiles),
        out_shape=(
            jax.ShapeDtypeStruct((everything, LANES), I32),
            jax.ShapeDtypeStruct((everything, LANES), I32),
            jax.ShapeDtypeStruct((8, everything), I32),
        ),
        scratch_shapes=[pltpu.VMEM((everything, LANES), I32)],
        cost_estimate=cost,
        compiler_params=params,
        name="index",
    )(keep)

    prefix, before = pl.pallas_call(
        functools.partial(head_kernel, count, tiles, group),
        in_specs=[smem, vmem, vmem],
        out_specs=[vmem, vmem],
        out_shape=[
            jax.ShapeDtypeStruct((everything, cols, LANES), F32),
            jax.ShapeDtypeStruct((8, width), F32),
        ],
        scratch_shapes=[
            pltpu.VMEM((8, width), F32),
            pltpu.VMEM((count, 8, width), F32),
            pltpu.SemaphoreType.DMA((count,)),
            pltpu.SemaphoreType.DMA((count,)),
        ],
        compiler_params=pltpu.CompilerParams(collective_id=0, has_side_effects=True, vmem_limit_bytes=GRANT),
        name="head",
    )(scalars, events, keep)

    tables, tails, sent = [], [], []
    for s in range(streams):
        table, send = pl.pallas_call(
            functools.partial(pack_kernel, s, tiles),
            in_specs=[smem, vmem, vmem] + [anywhere] * (s > 0),
            out_specs=[vmem, vmem],
            out_shape=[
                jax.ShapeDtypeStruct((tiles + 2, cols, LANES), F32),
                jax.ShapeDtypeStruct((back, cols, LANES), F32),
            ],
            cost_estimate=cost,
            compiler_params=params,
            name=f"pack{s}",
        )(scalars, prefix, slot, *tables[-1:])
        tails.append(lax.ppermute(send, "rows", [(i, i + 1) for i in range(count - 1)]))
        tables.append(table)

    outs = ()
    for s in range(streams):
        outs = pl.pallas_call(
            functools.partial(spread_kernel, s, tiles, group),
            in_specs=[smem] + [vmem] * 5 + [anywhere] * len(outs),
            out_specs=[anywhere] * 2,
            out_shape=[jax.ShapeDtypeStruct(events.shape, F32)] * 2,
            scratch_shapes=[
                pltpu.VMEM((cols, rows), F32),
                pltpu.VMEM((cols, rows), F32),
                pltpu.VMEM((tiles, LANES), F32),
                pltpu.SemaphoreType.DMA((2, tiles // group)),
            ],
            input_output_aliases={6: 0, 7: 1} if outs else {},
            cost_estimate=cost,
            compiler_params=params,
            name=f"spread{s}",
        )(scalars, before, rank, prefix, tables[s], tails[s], *outs)
    return tuple(outs)


def solution(mesh):
    return jax.shard_map(
        functools.partial(per_device, mesh.shape["rows"]),
        mesh=mesh,
        in_specs=(P(None, None, "rows"), P(None, "rows")),
        out_specs=(P(None, None, "rows"), P(None, None, "rows")),
        check_vma=False,
    )
```
